256 devices in a mesh: shadow: 32 (over z, y_lo, core), vocab: 8 (over y_hi, x).
Axes of the slice: x: 4, y: 4 (y_hi: 2, y_lo: 2; y = y_hi * 2 + y_lo), z: 8, core: 2. Of those that a mesh axis runs over, the one named last changes fastest.
Arguments:
- hidden: bfloat16 [128, 128, 2048], P('shadow'), may hold values from -18 to 18
- targets: int32 [128], replicated, may hold values from 0 to 32767
- membership: int32 [128, 4], P('shadow'), may hold values from 0 to 1, as said below
- unembedding: bfloat16 [32768, 2048], P(('shadow', 'vocab')), may hold values from -1 to 1
Outputs:
- score: float32 [128, 128], P('shadow', 'vocab')
The draws below stay inside these ranges and needn't reach their ends.
Inputs may be any that keep to these rules, and one draw needn't show every extreme that they name: `membership`: each candidate sequence is a member of exactly 64 of the shadow models.
All inputs are finite; a program needn't handle non-finite values.
Results may differ from the reference program's by a relative error of at most 0.00055.
Values may be sent and summed in bfloat16 or wider, within the bound.
No kernel may reach another device: no remote copies, remote signals or barrier semaphores. Data moves between devices by JAX's collectives and lax.ppermute only.
A program may use at most 64 MiB of HBM per device.

```python
import math
import jax
import jax.numpy as jnp
import numpy as np
from jax import lax

D = 2048
TOK = 128
SEQ = 32
SHADOWS = 128
VOCAB = 32768
EXAMPLES = 4


def head_table(key):
    unscaled = jax.random.truncated_normal(jax.random.fold_in(key, 11), -4.0, 4.0, (VOCAB, D), jnp.float32)
    return unscaled * D ** (-0.5)


def draw_unembedding(key, part):
    return head_table(key).astype(jnp.bfloat16)


def draw_hidden(key, part):
    states = jnp.clip(jax.random.normal(jax.random.fold_in(key, 12), (SHADOWS, TOK, D), jnp.float32), -4.0, 4.0)
    return states.astype(jnp.bfloat16)


def draw_membership(key, part):
    noise = jax.random.randint(jax.random.fold_in(key, 13), (SHADOWS, EXAMPLES), 0, 1 << 20, jnp.int32)
    noise = noise * SHADOWS + jnp.arange(SHADOWS, dtype=jnp.int32)[:, None]
    ordering = jnp.argsort(noise, axis=0)
    ranking = jnp.argsort(ordering, axis=0)
    return (ranking < SHADOWS // 2).astype(jnp.int32)


def touch_ends(array, own_key, low, high):
    longest = array.shape.index(max(array.shape))
    spots = []
    for shift in (0, 1):
        where = [jax.random.randint(jax.random.fold_in(own_key, axis), (), 0, length) for axis, length in enumerate(array.shape)]
        where[longest] = (where[longest] + shift) % array.shape[longest]
        spots.append(tuple(where))
    return array.at[spots[0]].set(low).at[spots[1]].set(high)


def cumulative_ranks(number_of, lean):
    loads = [(1 << 20) // math.isqrt(standing ** lean) + 1 for standing in range(1, number_of + 1)]
    spread = 1 + sum(loads) // (1 << 30)
    return np.cumsum(np.array([max(1, weight // spread) for weight in loads]))


def skewed_ids(key, shape, amount, skew):
    grid = cumulative_ranks(amount, skew)
    ticket = jax.random.randint(jax.random.fold_in(key, 1), shape, 0, int(grid[amount - 1]))
    rank = jnp.searchsorted(jnp.asarray(grid, jnp.int32), ticket, side="right")
    return jax.random.permutation(jax.random.fold_in(key, 2), amount)[rank].astype(jnp.int32)


def setup_inputs(seed: int = 0) -> dict:
    keys = jax.random.split(jax.random.key(seed), 5)
    hidden = draw_hidden(jax.random.fold_in(keys[4], 71), 0)
    targets = touch_ends(skewed_ids(keys[1], (TOK,), VOCAB, 2), jax.random.fold_in(keys[1], 3), 0, VOCAB - 1).astype(jnp.int32)
    membership = draw_membership(jax.random.fold_in(keys[4], 71), 0)
    unembedding = draw_unembedding(jax.random.fold_in(keys[4], 71), 0)
    return dict(hidden=hidden, targets=targets, membership=membership, unembedding=unembedding)


NEG_FILL = -1e+30
VAR_FLOOR = 0.5

def reference(hidden, targets, membership, unembedding):
    columns = jnp.arange(unembedding.shape[0], dtype=jnp.int32)
    target_hit = targets.astype(jnp.int32)[:, None] == columns[None, :]

    def confidence_of(states):
        logits = lax.dot_general(states, unembedding, (((1,), (1,)), ((), ())), preferred_element_type=jnp.float32)
        target_logit = lax.optimization_barrier(jnp.sum(jnp.where(target_hit, logits, 0.0), axis=1))
        others = jnp.where(target_hit, NEG_FILL, logits)
        highest = lax.optimization_barrier(jnp.max(others, axis=1))
        summed = lax.optimization_barrier(jnp.sum(jnp.where(target_hit, 0.0, jnp.exp(others - highest[:, None])), axis=1))
        return target_logit - (highest + jnp.log(summed))
    confidence = lax.map(confidence_of, hidden)
    outside = (1 - jnp.repeat(membership, SEQ, axis=1)).astype(jnp.float32)
    weighted = outside * confidence
    first_moment = lax.optimization_barrier(jnp.sum(weighted, axis=0))
    second_moment = lax.optimization_barrier(jnp.sum(weighted * confidence, axis=0))
    out_count = SHADOWS // 2 - outside
    out_mean = (first_moment[None, :] - weighted) / out_count
    out_variance = (second_moment[None, :] - weighted * confidence) / out_count - out_mean * out_mean
    return (confidence - out_mean) * lax.rsqrt(jnp.maximum(out_variance, 0.0) + VAR_FLOOR)
```

```python
import functools

import jax
import jax.numpy as jnp
from jax import lax
from jax.experimental import pallas as pl
from jax.experimental.pallas import tpu as pltpu
from jax.sharding import Mesh, PartitionSpec as P

SEQ = 32


NEG_FILL = -1e30
VAR_FLOOR = 0.5
PARTS = 2


def around(size, step):
    return [(k, (k + step) % size) for k in range(size)]


def y_around(step):
    place = lambda y: (y % 2) * 2 + y // 2
    return [(place(y), place((y + step) % 4)) for y in range(4)]


def scores_kernel(row_counts, head_count, first_ref, wanted_ref, *refs):
    block_refs, found = [], 0
    for counts in row_counts:
        block_refs.append(refs[found : found + len(counts)])
        found += len(counts)
    head_refs, out = refs[found : found + head_count], refs[-1]
    head = jnp.concatenate([ref[...] for ref in head_refs], axis=0)
    for b, counts in enumerate(row_counts):
        shadows = [(ref, k) for ref, count in zip(block_refs[b], counts) for k in range(count)]
        for half in range(2):
            rows = jnp.concatenate(
                [ref[k, 16 * v : 16 * v + 16, :] for v in range(4 * half, 4 * half + 4) for ref, k in shadows],
                axis=0,
            )
            logits = lax.dot_general(
                head, rows, (((1,), (1,)), ((), ())), preferred_element_type=jnp.float32
            )
            lanes = slice(256 * half, 256 * half + 256)
            wanted = wanted_ref[0:1, lanes]
            pieces, at = [], 0
            for k, ref in enumerate(head_refs):
                part = logits[at : at + ref.shape[0]]
                at += ref.shape[0]
                vocab_rows = lax.broadcasted_iota(jnp.int32, part.shape, 0) + first_ref[k]
                pieces.append((part, vocab_rows == wanted))
            target_logit = sum(
                jnp.sum(jnp.where(hit, part, 0.0), axis=0, keepdims=True) for part, hit in pieces
            )
            others = [jnp.where(hit, NEG_FILL, part) for part, hit in pieces]
            highest = functools.reduce(
                jnp.maximum, [jnp.max(part, axis=0, keepdims=True) for part in others]
            )
            summed = sum(
                jnp.sum(jnp.where(hit, 0.0, jnp.exp(part - highest)), axis=0, keepdims=True)
                for part, (_, hit) in zip(others, pieces)
            )
            out[b, 0:1, lanes] = highest
            out[b, 1:2, lanes] = summed
            out[b, 2:3, lanes] = target_logit


def score_blocks(blocks, pieces, wanted):
    heads = [head for head, _ in pieces]
    first = jnp.stack([start for _, start in pieces])
    flat = [rows for block in blocks for rows in block]
    vmem = pl.BlockSpec(memory_space=pltpu.VMEM)
    head_rows = sum(head.shape[0] for head in heads)
    return pl.pallas_call(
        functools.partial(
            scores_kernel, [[rows.shape[0] for rows in block] for block in blocks], len(heads)
        ),
        in_specs=[pl.BlockSpec(memory_space=pltpu.SMEM), vmem] + [vmem] * (len(flat) + len(heads)),
        out_specs=vmem,
        out_shape=jax.ShapeDtypeStruct((len(blocks), 3, 512), jnp.float32),
        compiler_params=pltpu.CompilerParams(vmem_limit_bytes=20 << 20),
        cost_estimate=pl.CostEstimate(
            flops=2 * 512 * len(blocks) * head_rows * 2048,
            bytes_accessed=2 * 2048 * head_rows,
            transcendentals=512 * len(blocks) * head_rows,
        ),
    )(first, wanted, *flat, *heads)


def after(values, others):
    return lax.optimization_barrier((*values, *others))[: len(values)]


def combine(earlier, latter):
    raised = jnp.maximum(earlier[:, 0], latter[:, 0])
    summed = earlier[:, 1] * jnp.exp(earlier[:, 0] - raised) + latter[:, 1] * jnp.exp(
        latter[:, 0] - raised
    )
    return jnp.stack([raised, summed, earlier[:, 2] + latter[:, 2]], axis=1)


def per_device(hidden, targets, membership, unembedding):
    shadow_count, token_count, model_width = hidden.shape
    head_rows = unembedding.shape[0]
    z, yl, core = lax.axis_index("z"), lax.axis_index("yl"), lax.axis_index("c")
    vocab_index = lax.axis_index(("yh", "x"))
    part_rows = head_rows // PARTS

    def first_row(step, part):
        source = (((z - step) % 8 * 2 + yl) * 2 + core) * 8 + vocab_index
        return source * head_rows + part * part_rows

    wanted = jnp.broadcast_to(
        targets.reshape(8, 1, token_count // 8), (8, shadow_count, token_count // 8)
    ).reshape(1, shadow_count * token_count)

    half = shadow_count // 2
    swap = [(0, 1), (1, 0)]
    up = [unembedding[k * part_rows : (k + 1) * part_rows] for k in range(PARTS)]
    down = list(up)
    gathered = [[(unembedding, first_row(0, 0))]]

    def forward(step):
        for k in range(PARTS):
            up[k] = lax.ppermute(up[k], "z", around(8, 1))
            down[k] = lax.ppermute(down[k], "z", around(8, -1))
        gathered.append(
            [(up[k], first_row(step, k)) for k in range(PARTS)]
            + [(down[k], first_row(-step, k)) for k in range(PARTS)]
        )

    forward(1)
    beside = lax.ppermute(hidden, "c", swap)
    low_half = lax.ppermute(hidden[:half], ("yl", "yh"), y_around(-1))
    high_half = lax.ppermute(hidden[half:], ("yl", "yh"), y_around(1))
    forward(2)
    near = [[hidden], [beside]]
    near_found = score_blocks(near, gathered[0] + gathered[1], wanted)
    low_half, high_half = after((low_half, high_half), (near_found, up[0], down[0]))
    across = jnp.concatenate([low_half, high_half])
    across_beside = lax.ppermute(across, "c", swap)
    forward(3)
    near_found = combine(near_found, score_blocks(near, gathered[2], wanted))
    across_beside, wanted_far = after((across_beside, wanted), (near_found, up[0]))
    far = [[across], [across_beside]]
    last = []
    for k in range(PARTS):
        if k < PARTS // 2:
            last.append((lax.ppermute(up[k], "z", around(8, 1)), first_row(4, k)))
        else:
            last.append((lax.ppermute(down[k], "z", around(8, -1)), first_row(4, k)))
    far_found = score_blocks(far, gathered[0] + gathered[1] + gathered[2], wanted_far)
    found = jnp.concatenate([near_found, far_found])
    found = combine(found, score_blocks(near + far, gathered[3], wanted_far))
    (wanted_last,) = after((wanted,), (found,))
    found = combine(found, score_blocks(near + far, last, wanted_last))

    both = jnp.stack([found[:, 0] + jnp.log(found[:, 1]), found[:, 2]], axis=1)
    both = both.reshape(2, 2, 2, 8, 64)
    both = jnp.where(yl == 1, both[::-1], both)
    both = jnp.where(core == 1, both[:, ::-1], both)
    message = both.transpose(0, 1, 3, 2, 4).reshape(32, 1, 128)
    received = lax.all_to_all(
        message, ("yl", "c", "yh", "x"), split_axis=0, concat_axis=0, tiled=True
    ).reshape(32, 128)
    partial, target_logit = received[:, :64], jnp.sum(received[:, 64:], axis=0)
    highest = jnp.max(partial, axis=0)
    summed = jnp.sum(jnp.exp(partial - highest[None]), axis=0)
    slice_tokens = token_count // 8
    confidence = (target_logit - (highest + jnp.log(summed))).reshape(shadow_count, slice_tokens)

    member_tokens = jnp.repeat(membership, SEQ, axis=1)
    outside = (
        1 - lax.dynamic_slice_in_dim(member_tokens, vocab_index * slice_tokens, slice_tokens, 1)
    ).astype(jnp.float32)
    weighted = outside * confidence
    sums = jnp.concatenate([jnp.sum(weighted, axis=0), jnp.sum(weighted * confidence, axis=0)])
    copies = jnp.broadcast_to(sums, (32, 1, 2 * slice_tokens))
    total = jnp.sum(
        lax.all_to_all(copies, ("z", "yl", "c"), split_axis=0, concat_axis=0, tiled=True), axis=(0, 1)
    )
    first_moment, second_moment = total[:slice_tokens], total[slice_tokens:]
    out_count = 64 - outside
    out_mean = (first_moment[None, :] - weighted) / out_count
    out_variance = (
        second_moment[None, :] - weighted * confidence
    ) / out_count - out_mean * out_mean
    return (confidence - out_mean) * lax.rsqrt(jnp.maximum(out_variance, 0.0) + VAR_FLOOR)


def solution(mesh):
    parts = Mesh(mesh.devices.reshape(8, 2, 2, 2, 4), ("z", "yl", "c", "yh", "x"))
    shadow, vocab = ("z", "yl", "c"), ("yh", "x")
    return jax.shard_map(
        per_device,
        mesh=parts,
        in_specs=(P(shadow, None, None), P(), P(shadow, None), P(shadow + vocab, None)),
        out_specs=P(shadow, vocab),
        check_vma=False,
    )
```

```python
import functools

import jax
import jax.numpy as jnp
from jax import lax
from jax.experimental import pallas as pl
from jax.experimental.pallas import tpu as pltpu
from jax.sharding import Mesh, PartitionSpec as P


SEQ = 32


NEG_FILL = -1e30
VAR_FLOOR = 0.5
PARTS = 2


def around(size, step):
    return [(k, (k + step) % size) for k in range(size)]


def across_y():
    place = lambda y, core: (y % 2 * 2 + core) * 2 + y // 2
    return [(place(y, core), place((y + 2 * core - 1) % 4, core)) for y in range(4) for core in (0, 1)]


def scores_kernel(fresh_counts, held, blocks, places, *refs):
    refs = list(refs)
    first_ref, wanted_ref = refs.pop(0), refs.pop(0)
    stores = {b: refs.pop(0) for b in held}
    fresh_refs = {b: refs.pop(0) for b in fresh_counts}
    head_refs = [refs.pop(0) for _ in places]
    out = refs.pop(0)
    copies = {}
    if fresh_counts:
        stores[min(fresh_counts)], sems = refs
        for b, ref in fresh_refs.items():
            for half in range(2):
                tokens = pl.ds(64 * half, 64)
                copies[b, half] = pltpu.make_async_copy(
                    ref.at[:, tokens],
                    stores[b - b % 2].at[b % 2, :, tokens],
                    sems.at[len(copies)],
                )
        queue = list(copies.values())
        for copy in queue[:2]:
            copy.start()
        queue = queue[2:]
    groups, sizes = [[]], [0]
    for place, ref in zip(places, head_refs):
        if sizes[-1] + ref.shape[0] > 256:
            groups.append([])
            sizes.append(0)
        groups[-1].append((place, ref))
        sizes[-1] += ref.shape[0]
    for n, b in enumerate(blocks):
        for half in range(2):
            if copies:
                copies[b, half].wait()
                if queue:
                    queue.pop(0).start()
            rows = jnp.concatenate(
                [
                    stores[b - b % 2][b % 2, k, 16 * v : 16 * v + 16, :]
                    for v in range(4 * half, 4 * half + 4)
                    for k in range(4)
                ],
                axis=0,
            )
            lanes = slice(256 * half, 256 * half + 256)
            wanted = wanted_ref[0:1, lanes]
            pieces = []
            for group in groups:
                head = jnp.concatenate([ref[...] for _, ref in group], axis=0)
                logits = lax.dot_general(
                    head, rows, (((1,), (1,)), ((), ())), preferred_element_type=jnp.float32
                )
                at = 0
                for place, ref in group:
                    part = logits[at : at + ref.shape[0]]
                    at += ref.shape[0]
                    vocab_rows = lax.broadcasted_iota(jnp.int32, part.shape, 0) + first_ref[place]
                    pieces.append((part, vocab_rows == wanted))
            target_logit = sum(
                jnp.sum(jnp.where(hit, part, 0.0), axis=0, keepdims=True) for part, hit in pieces
            )
            others = [jnp.where(hit, NEG_FILL, part) for part, hit in pieces]
            highest = functools.reduce(
                jnp.maximum, [jnp.max(part, axis=0, keepdims=True) for part in others]
            )
            summed = sum(
                jnp.sum(jnp.exp(part - highest), axis=0, keepdims=True) for part in others
            )
            out[n, 0:1, lanes] = highest
            out[n, 1:2, lanes] = summed
            out[n, 2:3, lanes] = target_logit


def score_blocks(stores, fresh, blocks, pieces, first, wanted):
    heads = [head for head, _ in pieces]
    vmem = pl.BlockSpec(memory_space=pltpu.VMEM)
    head_rows = sum(head.shape[0] for head in heads)
    outs = [jax.ShapeDtypeStruct((len(blocks), 3, 512), jnp.float32)]
    if fresh:
        outs.append(jax.ShapeDtypeStruct((2, 4, 128, 2048), jnp.bfloat16))
    results = pl.pallas_call(
        functools.partial(
            scores_kernel, list(fresh), list(stores), blocks, [place for _, place in pieces]
        ),
        in_specs=[pl.BlockSpec(memory_space=pltpu.SMEM), vmem]
        + [vmem] * len(stores)
        + [pl.BlockSpec(memory_space=pltpu.HBM)] * len(fresh)
        + [vmem] * len(heads),
        out_specs=[vmem] * len(outs),
        out_shape=outs,
        scratch_shapes=[pltpu.SemaphoreType.DMA((4,))] if fresh else [],
        compiler_params=pltpu.CompilerParams(vmem_limit_bytes=12 << 20),
        cost_estimate=pl.CostEstimate(
            flops=2 * 512 * len(blocks) * head_rows * 2048,
            bytes_accessed=2 * 2048 * (head_rows + 512 * len(blocks)),
            transcendentals=512 * len(blocks) * head_rows,
        ),
    )(
        first,
        wanted,
        *stores.values(),
        *[pltpu.with_memory_space_constraint(rows, pltpu.HBM) for rows in fresh.values()],
        *heads,
    )
    return results


def wanted_kernel(targets_ref, wanted_ref):
    targets = jnp.broadcast_to(targets_ref[...], (8, 128))
    turned = [targets] + [pltpu.roll(targets, 16 * k, 1) for k in range(1, 8)]
    place = lax.broadcasted_iota(jnp.int32, (8, 128), 1) // 16
    for quarter in range(4):
        lanes = targets
        for s in range(8):
            lanes = jnp.where(place == s, turned[(s - 2 * quarter - s // 4) % 8], lanes)
        wanted_ref[0:1, 128 * quarter : 128 * quarter + 128] = lanes[0:1]


def wanted_rows(targets):
    vmem = pl.BlockSpec(memory_space=pltpu.VMEM)
    return pl.pallas_call(
        wanted_kernel,
        in_specs=[vmem],
        out_specs=vmem,
        out_shape=jax.ShapeDtypeStruct((1, 512), jnp.int32),
        compiler_params=pltpu.CompilerParams(vmem_limit_bytes=4 << 20),
    )(targets.reshape(1, 128))


def after(values, others):
    return lax.optimization_barrier((*values, *others))[: len(values)]


def combine(earlier, latter):
    raised = jnp.maximum(earlier[:, 0], latter[:, 0])
    summed = earlier[:, 1] * jnp.exp(earlier[:, 0] - raised) + latter[:, 1] * jnp.exp(
        latter[:, 0] - raised
    )
    return jnp.stack([raised, summed, earlier[:, 2] + latter[:, 2]], axis=1)


def per_device(hidden, targets, membership, unembedding):
    shadow_count, token_count, _ = hidden.shape
    head_rows = unembedding.shape[0]
    z, yl, core = lax.axis_index("z"), lax.axis_index("yl"), lax.axis_index("c")
    vocab_index = lax.axis_index(("yh", "x"))
    part_rows = head_rows // PARTS

    place = jnp.arange(8 * PARTS, dtype=jnp.int32)
    source = (((z - place // PARTS) & 7) * 4 + yl * 2 + core) * 8 + vocab_index
    first = source * head_rows + place % PARTS * part_rows

    swap = [(0, 1), (1, 0)]
    up = [unembedding[k * part_rows : (k + 1) * part_rows] for k in range(PARTS)]
    down = list(up)
    gathered = [[(unembedding, 0)]]

    def forward(step):
        for k in range(PARTS):
            up[k] = lax.ppermute(up[k], "z", around(8, 1))
            down[k] = lax.ppermute(down[k], "z", around(8, -1))
        gathered.append(
            [(up[k], PARTS * step + k) for k in range(PARTS)]
            + [(down[k], PARTS * (8 - step) + k) for k in range(PARTS)]
        )

    forward(1)
    beside = lax.ppermute(hidden, "c", swap)
    across = lax.ppermute(hidden, ("yl", "c", "yh"), across_y())
    wanted = wanted_rows(targets)
    forward(2)
    near_found, near = score_blocks({}, {0: hidden, 1: beside}, [0, 1], gathered[1], first, wanted)
    forward(3)
    diagonal = lax.ppermute(across, "c", swap)
    (latter,) = score_blocks({0: near}, {}, [0, 1], gathered[2], first, wanted)
    near_found = combine(near_found, latter)
    last = []
    for k in range(PARTS):
        if k < PARTS // 2:
            last.append((lax.ppermute(up[k], "z", around(8, 1)), PARTS * 4 + k))
        else:
            last.append((lax.ppermute(down[k], "z", around(8, -1)), PARTS * 4 + k))
    (wanted_far,) = after((wanted,), (near_found,))
    far_found, far = score_blocks(
        {}, {2: across, 3: diagonal}, [2, 3], gathered[1] + gathered[2], first, wanted_far
    )
    found = jnp.concatenate([near_found, far_found])
    stores, every = {0: near, 2: far}, [0, 1, 2, 3]
    (latter,) = score_blocks(stores, {}, every, gathered[3], first, wanted_far)
    found = combine(found, latter)
    (wanted_last,) = after((wanted,), (found,))
    (latter,) = score_blocks(stores, {}, every, gathered[0] + last, first, wanted_last)
    found = combine(found, latter)

    both = jnp.stack([found[:, 0] + jnp.log(found[:, 1]), found[:, 2]], axis=1)
    both = both.reshape(2, 2, 2, 8, 64)
    both = jnp.where(yl == 1, both[::-1], both)
    both = jnp.where(core == 1, both[:, ::-1], both)
    message = both.transpose(0, 1, 3, 2, 4).reshape(32, 1, 128)
    received = lax.all_to_all(
        message, ("yl", "c", "yh", "x"), split_axis=0, concat_axis=0, tiled=True
    ).reshape(32, 128)
    partial, target_logit = received[:, :64], jnp.sum(received[:, 64:], axis=0)
    highest = jnp.max(partial, axis=0)
    summed = jnp.sum(jnp.exp(partial - highest[None]), axis=0)
    slice_tokens = token_count // 8
    confidence = (target_logit - (highest + jnp.log(summed))).reshape(shadow_count, slice_tokens)

    member_tokens = jnp.repeat(membership, SEQ, axis=1)
    outside = (
        1 - lax.dynamic_slice_in_dim(member_tokens, vocab_index * slice_tokens, slice_tokens, 1)
    ).astype(jnp.float32)
    weighted = outside * confidence
    sums = jnp.concatenate([jnp.sum(weighted, axis=0), jnp.sum(weighted * confidence, axis=0)])
    copies = jnp.broadcast_to(sums, (32, 1, 2 * slice_tokens))
    total = jnp.sum(
        lax.all_to_all(copies, ("z", "yl", "c"), split_axis=0, concat_axis=0, tiled=True), axis=(0, 1)
    )
    first_moment, second_moment = total[:slice_tokens], total[slice_tokens:]
    out_count = 64 - outside
    out_mean = (first_moment[None, :] - weighted) / out_count
    out_variance = (
        second_moment[None, :] - weighted * confidence
    ) / out_count - out_mean * out_mean
    return (confidence - out_mean) * lax.rsqrt(jnp.maximum(out_variance, 0.0) + VAR_FLOOR)


def solution(mesh):
    parts = Mesh(mesh.devices.reshape(8, 2, 2, 2, 4), ("z", "yl", "c", "yh", "x"))
    shadow, vocab = ("z", "yl", "c"), ("yh", "x")

    return jax.shard_map(
        per_device,
        mesh=parts,
        in_specs=(P(shadow, None, None), P(), P(shadow, None), P(shadow + vocab, None)),
        out_specs=P(shadow, vocab),
        check_vma=False,
    )
```

```python
import functools

import jax
import jax.numpy as jnp
from jax import lax
from jax.experimental import pallas as pl
from jax.experimental.pallas import tpu as pltpu
from jax.sharding import Mesh, PartitionSpec as P


SEQ = 32


NEG_FILL = -1e30
VAR_FLOOR = 0.5
PARTS = 2


def around(size, step):
    return [(k, (k + step) % size) for k in range(size)]


def across_y():
    place = lambda y, core: (y % 2 * 2 + core) * 2 + y // 2
    return [(place(y, core), place((y + 2 * core - 1) % 4, core)) for y in range(4) for core in (0, 1)]


def scores_kernel(done_near, before_count, fresh_counts, held, blocks, places, *refs):
    refs = list(refs)
    first_ref, wanted_ref = refs.pop(0), refs.pop(0)
    before = [refs.pop(0) for _ in range(before_count)]
    place_of = {}
    for group in held:
        ref = refs.pop(0)
        place_of |= {b: ref.at[n] if len(ref.shape) == 4 else ref for n, b in enumerate(group)}
    fresh_refs = {b: refs.pop(0) for b in fresh_counts}
    head_refs = [refs.pop(0) for _ in places]
    out = refs.pop(0)
    copies = {}
    if fresh_counts:
        kept, sems = refs
        place_of |= {b: kept.at[n] for n, b in enumerate(fresh_counts)}
        for b, ref in fresh_refs.items():
            for half in range(2):
                tokens = pl.ds(64 * half, 64)
                copies[b, half] = pltpu.make_async_copy(
                    ref.at[:, tokens],
                    place_of[b].at[:, tokens],
                    sems.at[len(copies)],
                )
        queue = list(copies.values())
        for copy in queue[:2]:
            copy.start()
        queue = queue[2:]

    def grouped(b):
        groups, size = [[]], 0
        for place, ref in zip(places, head_refs):
            if b < 2 and place in done_near:
                continue
            if size + ref.shape[0] > 256:
                groups.append([])
                size = 0
            groups[-1].append((place, ref))
            size += ref.shape[0]
        return groups

    for n, b in enumerate(blocks):
        for half in range(2):
            if (b, half) in copies:
                copies[b, half].wait()
                if queue:
                    queue.pop(0).start()
            rows = jnp.concatenate(
                [
                    place_of[b][k, 16 * v : 16 * v + 16, :]
                    for v in range(4 * half, 4 * half + 4)
                    for k in range(4)
                ],
                axis=0,
            )
            lanes = slice(256 * half, 256 * half + 256)
            wanted = wanted_ref[0:1, lanes]
            pieces = []
            for group in grouped(b):
                head = jnp.concatenate([ref[...] for _, ref in group], axis=0)
                logits = lax.dot_general(
                    head, rows, (((1,), (1,)), ((), ())), preferred_element_type=jnp.float32
                )
                at = 0
                for place, ref in group:
                    part = logits[at : at + ref.shape[0]]
                    at += ref.shape[0]
                    vocab_rows = lax.broadcasted_iota(jnp.int32, part.shape, 0) + first_ref[place]
                    pieces.append((part, vocab_rows == wanted))
            target_logit = sum(
                jnp.sum(jnp.where(hit, part, 0.0), axis=0, keepdims=True) for part, hit in pieces
            )
            others = [jnp.where(hit, NEG_FILL, part) for part, hit in pieces]
            highest = functools.reduce(
                jnp.maximum, [jnp.max(part, axis=0, keepdims=True) for part in others]
            )
            summed = sum(
                jnp.sum(jnp.exp(part - highest), axis=0, keepdims=True) for part in others
            )
            if not before:
                out[n, 0:1, lanes] = highest
                out[n, 1:2, lanes] = summed
                out[n, 2:3, lanes] = target_logit
                continue
            for ref in before:
                earlier, raised = ref[n, 0:1, lanes], jnp.maximum(highest, ref[n, 0:1, lanes])
                summed = summed * jnp.exp(highest - raised) + ref[n, 1:2, lanes] * jnp.exp(
                    earlier - raised
                )
                highest = raised
                target_logit = target_logit + ref[n, 2:3, lanes]
            total, message = highest + jnp.log(summed), []
            left = lax.broadcasted_iota(jnp.int32, (1, 128), 1) < 64
            for k in range(2):
                part, hit = total[:, 128 * k : 128 * k + 128], target_logit[:, 128 * k : 128 * k + 128]
                message.append(jnp.where(left, part, pltpu.roll(hit, 64, 1)))
                message.append(jnp.where(left, pltpu.roll(part, 64, 1), hit))
            owner = first_ref[first_ref.shape[0] - 1] ^ b
            out[owner, 4 * half : 4 * half + 4, :] = jnp.concatenate(message, axis=0)


def score_blocks(stores, fresh, blocks, pieces, first, wanted, before=(), done_near=()):
    heads = [head for head, _ in pieces]
    vmem = pl.BlockSpec(memory_space=pltpu.VMEM)
    head_rows = sum(head.shape[0] for head in heads)
    shape = (4, 8, 128) if before else (len(blocks), 3, 512)
    outs = [jax.ShapeDtypeStruct(shape, jnp.float32)]
    if fresh:
        outs.append(jax.ShapeDtypeStruct((len(fresh), 4, 128, 2048), jnp.bfloat16))
    results = pl.pallas_call(
        functools.partial(
            scores_kernel, done_near, len(before), list(fresh), list(stores), blocks, [place for _, place in pieces]
        ),
        in_specs=[pl.BlockSpec(memory_space=pltpu.SMEM), vmem]
        + [vmem] * (len(before) + len(stores))
        + [pl.BlockSpec(memory_space=pltpu.HBM)] * len(fresh)
        + [vmem] * len(heads),
        out_specs=[vmem] * len(outs),
        out_shape=outs,
        scratch_shapes=[pltpu.SemaphoreType.DMA((2 * len(fresh),))] if fresh else [],
        compiler_params=pltpu.CompilerParams(vmem_limit_bytes=12 << 20),
        cost_estimate=pl.CostEstimate(
            flops=2 * 512 * len(blocks) * head_rows * 2048,
            bytes_accessed=2 * 2048 * (head_rows + 512 * len(blocks)),
            transcendentals=512 * len(blocks) * head_rows,
        ),
    )(
        first,
        wanted,
        *before,
        *stores.values(),
        *[pltpu.with_memory_space_constraint(rows, pltpu.HBM) for rows in fresh.values()],
        *heads,
    )
    return results


def wanted_kernel(targets_ref, wanted_ref):
    targets = jnp.broadcast_to(targets_ref[...], (8, 128))
    turned = [targets] + [pltpu.roll(targets, 16 * k, 1) for k in range(1, 8)]
    place = lax.broadcasted_iota(jnp.int32, (8, 128), 1) // 16
    for quarter in range(4):
        lanes = targets
        for s in range(8):
            lanes = jnp.where(place == s, turned[(s - 2 * quarter - s // 4) % 8], lanes)
        wanted_ref[0:1, 128 * quarter : 128 * quarter + 128] = lanes[0:1]


def wanted_rows(targets):
    vmem = pl.BlockSpec(memory_space=pltpu.VMEM)
    return pl.pallas_call(
        wanted_kernel,
        in_specs=[vmem],
        out_specs=vmem,
        out_shape=jax.ShapeDtypeStruct((1, 512), jnp.int32),
        compiler_params=pltpu.CompilerParams(vmem_limit_bytes=4 << 20),
    )(targets.reshape(1, 128))


def after(values, others):
    return lax.optimization_barrier((*values, *others))[: len(values)]


def combine(earlier, latter):
    raised = jnp.maximum(earlier[:, 0], latter[:, 0])
    summed = earlier[:, 1] * jnp.exp(earlier[:, 0] - raised) + latter[:, 1] * jnp.exp(
        latter[:, 0] - raised
    )
    return jnp.stack([raised, summed, earlier[:, 2] + latter[:, 2]], axis=1)


def per_device(hidden, targets, membership, unembedding):
    shadow_count, token_count, _ = hidden.shape
    head_rows = unembedding.shape[0]
    z, yl, core = lax.axis_index("z"), lax.axis_index("yl"), lax.axis_index("c")
    vocab_index = lax.axis_index(("yh", "x"))
    part_rows = head_rows // PARTS

    place = jnp.arange(8 * PARTS + 1, dtype=jnp.int32)
    source = (((z - place // PARTS) & 7) * 4 + yl * 2 + core) * 8 + vocab_index
    first = source * head_rows + place % PARTS * part_rows
    first = jnp.where(jnp.arange(8 * PARTS + 1) < 8 * PARTS, first, yl * 2 + core)

    swap = [(0, 1), (1, 0)]
    up, down, gathered = [unembedding], [unembedding], [[(unembedding, 0)]]

    def forward(step):
        for k in range(len(up)):
            up[k] = lax.ppermute(up[k], "z", around(8, 1))
            down[k] = lax.ppermute(down[k], "z", around(8, -1))
        gathered.append(
            [(rows, PARTS * step + k) for k, rows in enumerate(up)]
            + [(rows, PARTS * (8 - step) + k) for k, rows in enumerate(down)]
        )

    forward(1)
    beside = lax.ppermute(hidden, "c", swap)
    across = lax.ppermute(hidden, ("yl", "c", "yh"), across_y())
    wanted = wanted_rows(targets)
    near_found, near = score_blocks({(1,): beside}, {0: hidden}, [1, 0], gathered[0], first, wanted)
    up = [up[0][k * part_rows : (k + 1) * part_rows] for k in range(PARTS)]
    down = [down[0][k * part_rows : (k + 1) * part_rows] for k in range(PARTS)]
    forward(2)
    held = {(0,): near, (1,): beside}
    (latter,) = score_blocks(held, {}, [0, 1], gathered[1], first, wanted)
    near_found = combine(near_found[::-1], latter)
    forward(3)
    diagonal = lax.ppermute(across, "c", swap)
    (latter,) = score_blocks(held, {}, [0, 1], gathered[2], first, wanted)
    near_found = combine(near_found, latter)
    last = []
    for k in range(PARTS):
        if k < PARTS // 2:
            last.append((lax.ppermute(up[k], "z", around(8, 1)), PARTS * 4 + k))
        else:
            last.append((lax.ppermute(down[k], "z", around(8, -1)), PARTS * 4 + k))
    early = gathered[1] + gathered[2]
    (wanted_far,) = after((wanted,), (near_found,))
    far_found, far = score_blocks({(3,): diagonal}, {2: across}, [3, 2], early, first, wanted_far)
    found = jnp.concatenate([near_found, far_found[::-1]])
    stores, every = held | {(2,): far, (3,): diagonal}, [0, 1, 2, 3]
    (latter,) = score_blocks(stores, {}, every, gathered[3], first, wanted_far)
    (wanted_last,) = after((wanted,), (latter,))
    (message,) = score_blocks(
        stores, {}, every, gathered[0] + last, first, wanted_last, (found, latter), (0,)
    )
    message = message.reshape(32, 1, 128)
    received = lax.all_to_all(
        message, ("yl", "c", "yh", "x"), split_axis=0, concat_axis=0, tiled=True
    ).reshape(32, 128)
    partial, target_logit = received[:, :64], jnp.sum(received[:, 64:], axis=0)
    highest = jnp.max(partial, axis=0)
    summed = jnp.sum(jnp.exp(partial - highest[None]), axis=0)
    slice_tokens = token_count // 8
    confidence = (target_logit - (highest + jnp.log(summed))).reshape(shadow_count, slice_tokens)

    member_tokens = jnp.repeat(membership, SEQ, axis=1)
    outside = (
        1 - lax.dynamic_slice_in_dim(member_tokens, vocab_index * slice_tokens, slice_tokens, 1)
    ).astype(jnp.float32)
    weighted = outside * confidence
    sums = jnp.concatenate([jnp.sum(weighted, axis=0), jnp.sum(weighted * confidence, axis=0)])
    copies = jnp.broadcast_to(sums, (32, 1, 2 * slice_tokens))
    total = jnp.sum(
        lax.all_to_all(copies, ("z", "yl", "c"), split_axis=0, concat_axis=0, tiled=True), axis=(0, 1)
    )
    first_moment, second_moment = total[:slice_tokens], total[slice_tokens:]
    out_count = 64 - outside
    out_mean = (first_moment[None, :] - weighted) / out_count
    out_variance = (
        second_moment[None, :] - weighted * confidence
    ) / out_count - out_mean * out_mean
    return (confidence - out_mean) * lax.rsqrt(jnp.maximum(out_variance, 0.0) + VAR_FLOOR)


def solution(mesh):
    parts = Mesh(mesh.devices.reshape(8, 2, 2, 2, 4), ("z", "yl", "c", "yh", "x"))
    shadow, vocab = ("z", "yl", "c"), ("yh", "x")

    return jax.shard_map(
        per_device,
        mesh=parts,
        in_specs=(P(shadow, None, None), P(), P(shadow, None), P(shadow + vocab, None)),
        out_specs=P(shadow, vocab),
        check_vma=False,
    )
```

```python
import functools

import jax
import jax.numpy as jnp
from jax import lax
from jax.experimental import pallas as pl
from jax.experimental.pallas import tpu as pltpu
from jax.sharding import Mesh, PartitionSpec as P


SEQ = 32


NEG_FILL = -1e30
VAR_FLOOR = 0.5
PARTS = 2


def around(size, step):
    return [(k, (k + step) % size) for k in range(size)]


def across_y():
    place = lambda y, core: (y % 2 * 2 + core) * 2 + y // 2
    return [(place(y, core), place((y + 2 * core - 1) % 4, core)) for y in range(4) for core in (0, 1)]


def scores_kernel(done_near, before_count, fresh_counts, held, blocks, places, *refs):
    refs = list(refs)
    first_ref, wanted_ref = refs.pop(0), refs.pop(0)
    before = [refs.pop(0) for _ in range(before_count)]
    place_of = {}
    for group in held:
        ref = refs.pop(0)
        place_of |= {b: ref.at[n] if len(ref.shape) == 4 else ref for n, b in enumerate(group)}
    fresh_refs = {b: refs.pop(0) for b in fresh_counts}
    head_refs = [refs.pop(0) for _ in places]
    out = refs.pop(0)
    copies = {}
    if fresh_counts:
        kept, sems = refs
        place_of |= {b: kept.at[n] for n, b in enumerate(fresh_counts)}
        for b, ref in fresh_refs.items():
            for half in range(2):
                tokens = pl.ds(64 * half, 64)
                copies[b, half] = pltpu.make_async_copy(
                    ref.at[:, tokens],
                    place_of[b].at[:, tokens],
                    sems.at[len(copies)],
                )
        queue = list(copies.values())
        for copy in queue[:2]:
            copy.start()
        queue = queue[2:]

    def grouped(b):
        groups, size = [[]], 0
        for place, ref in zip(places, head_refs):
            if b < 2 and place in done_near:
                continue
            if size + ref.shape[0] > 256:
                groups.append([])
                size = 0
            groups[-1].append((place, ref))
            size += ref.shape[0]
        return groups

    for b in blocks:
        n = sorted(blocks).index(b)
        for half in range(2):
            if (b, half) in copies:
                copies[b, half].wait()
                if queue:
                    queue.pop(0).start()
            rows = jnp.concatenate(
                [
                    place_of[b][k, 16 * v : 16 * v + 16, :]
                    for v in range(4 * half, 4 * half + 4)
                    for k in range(4)
                ],
                axis=0,
            )
            lanes = slice(256 * half, 256 * half + 256)
            wanted = wanted_ref[0:1, lanes]
            pieces = []
            for group in grouped(b):
                head = jnp.concatenate([ref[...] for _, ref in group], axis=0)
                logits = lax.dot_general(
                    head, rows, (((1,), (1,)), ((), ())), preferred_element_type=jnp.float32
                )
                at = 0
                for place, ref in group:
                    part = logits[at : at + ref.shape[0]]
                    at += ref.shape[0]
                    vocab_rows = lax.broadcasted_iota(jnp.int32, part.shape, 0) + first_ref[place]
                    pieces.append((part, vocab_rows == wanted))
            target_logit = sum(
                jnp.sum(jnp.where(hit, part, 0.0), axis=0, keepdims=True) for part, hit in pieces
            )
            others = [jnp.where(hit, NEG_FILL, part) for part, hit in pieces]
            highest = functools.reduce(
                jnp.maximum, [jnp.max(part, axis=0, keepdims=True) for part in others]
            )
            summed = sum(
                jnp.sum(jnp.exp(part - highest), axis=0, keepdims=True) for part in others
            )
            if not before:
                out[n, 0:1, lanes] = highest
                out[n, 1:2, lanes] = summed
                out[n, 2:3, lanes] = target_logit
                continue
            for ref in before:
                earlier, raised = ref[n, 0:1, lanes], jnp.maximum(highest, ref[n, 0:1, lanes])
                summed = summed * jnp.exp(highest - raised) + ref[n, 1:2, lanes] * jnp.exp(
                    earlier - raised
                )
                highest = raised
                target_logit = target_logit + ref[n, 2:3, lanes]
            total, message = highest + jnp.log(summed), []
            left = lax.broadcasted_iota(jnp.int32, (1, 128), 1) < 64
            for k in range(2):
                part, hit = total[:, 128 * k : 128 * k + 128], target_logit[:, 128 * k : 128 * k + 128]
                message.append(jnp.where(left, part, pltpu.roll(hit, 64, 1)))
                message.append(jnp.where(left, pltpu.roll(part, 64, 1), hit))
            owner = first_ref[first_ref.shape[0] - 1] ^ b
            out[owner, 4 * half : 4 * half + 4, :] = jnp.concatenate(message, axis=0)


def score_blocks(stores, fresh, blocks, pieces, first, wanted, before=(), done_near=()):
    heads = [head for head, _ in pieces]
    vmem = pl.BlockSpec(memory_space=pltpu.VMEM)
    head_rows = sum(head.shape[0] for head in heads)
    shape = (4, 8, 128) if before else (len(blocks), 3, 512)
    outs = [jax.ShapeDtypeStruct(shape, jnp.float32)]
    if fresh:
        outs.append(jax.ShapeDtypeStruct((len(fresh), 4, 128, 2048), jnp.bfloat16))
    results = pl.pallas_call(
        functools.partial(
            scores_kernel, done_near, len(before), list(fresh), list(stores), blocks, [place for _, place in pieces]
        ),
        in_specs=[pl.BlockSpec(memory_space=pltpu.SMEM), vmem]
        + [vmem] * (len(before) + len(stores))
        + [pl.BlockSpec(memory_space=pltpu.HBM)] * len(fresh)
        + [vmem] * len(heads),
        out_specs=[vmem] * len(outs),
        out_shape=outs,
        scratch_shapes=[pltpu.SemaphoreType.DMA((2 * len(fresh),))] if fresh else [],
        compiler_params=pltpu.CompilerParams(vmem_limit_bytes=12 << 20),
        cost_estimate=pl.CostEstimate(
            flops=2 * 512 * len(blocks) * head_rows * 2048,
            bytes_accessed=2 * 2048 * (head_rows + 512 * len(blocks)),
            transcendentals=512 * len(blocks) * head_rows,
        ),
    )(
        first,
        wanted,
        *before,
        *stores.values(),
        *[pltpu.with_memory_space_constraint(rows, pltpu.HBM) for rows in fresh.values()],
        *heads,
    )
    return results


def wanted_kernel(targets_ref, wanted_ref):
    targets = jnp.broadcast_to(targets_ref[...], (8, 128))
    turned = [targets] + [pltpu.roll(targets, 16 * k, 1) for k in range(1, 8)]
    place = lax.broadcasted_iota(jnp.int32, (8, 128), 1) // 16
    for quarter in range(4):
        lanes = targets
        for s in range(8):
            lanes = jnp.where(place == s, turned[(s - 2 * quarter - s // 4) % 8], lanes)
        wanted_ref[0:1, 128 * quarter : 128 * quarter + 128] = lanes[0:1]


def wanted_rows(targets):
    vmem = pl.BlockSpec(memory_space=pltpu.VMEM)
    return pl.pallas_call(
        wanted_kernel,
        in_specs=[vmem],
        out_specs=vmem,
        out_shape=jax.ShapeDtypeStruct((1, 512), jnp.int32),
        compiler_params=pltpu.CompilerParams(vmem_limit_bytes=4 << 20),
    )(targets.reshape(1, 128))


def after(values, others):
    return lax.optimization_barrier((*values, *others))[: len(values)]


def combine(earlier, latter):
    raised = jnp.maximum(earlier[:, 0], latter[:, 0])
    summed = earlier[:, 1] * jnp.exp(earlier[:, 0] - raised) + latter[:, 1] * jnp.exp(
        latter[:, 0] - raised
    )
    return jnp.stack([raised, summed, earlier[:, 2] + latter[:, 2]], axis=1)


def per_device(hidden, targets, membership, unembedding):
    shadow_count, token_count, _ = hidden.shape
    head_rows = unembedding.shape[0]
    z, yl, core = lax.axis_index("z"), lax.axis_index("yl"), lax.axis_index("c")
    vocab_index = lax.axis_index(("yh", "x"))
    part_rows = head_rows // PARTS

    place = jnp.arange(8 * PARTS + 1, dtype=jnp.int32)
    source = (((z - place // PARTS) & 7) * 4 + yl * 2 + core) * 8 + vocab_index
    first = source * head_rows + place % PARTS * part_rows
    first = jnp.where(jnp.arange(8 * PARTS + 1) < 8 * PARTS, first, yl * 2 + core)

    swap = [(0, 1), (1, 0)]
    up, down, gathered = [unembedding], [unembedding], [[(unembedding, 0)]]

    def forward(step):
        for k in range(len(up)):
            up[k] = lax.ppermute(up[k], "z", around(8, 1))
            down[k] = lax.ppermute(down[k], "z", around(8, -1))
        gathered.append(
            [(rows, PARTS * step + k) for k, rows in enumerate(up)]
            + [(rows, PARTS * (8 - step) + k) for k, rows in enumerate(down)]
        )

    forward(1)
    beside = lax.ppermute(hidden, "c", swap)
    across = lax.ppermute(hidden, ("yl", "c", "yh"), across_y())
    wanted = wanted_rows(targets)
    near_found, near = score_blocks({(1,): beside}, {0: hidden}, [1, 0], gathered[0], first, wanted)
    up = [up[0][k * part_rows : (k + 1) * part_rows] for k in range(PARTS)]
    down = [down[0][k * part_rows : (k + 1) * part_rows] for k in range(PARTS)]
    forward(2)
    held = {(0,): near, (1,): beside}
    (latter,) = score_blocks(held, {}, [0, 1], gathered[1], first, wanted)
    near_found = combine(near_found, latter)
    forward(3)
    diagonal = lax.ppermute(across, "c", swap)
    (latter,) = score_blocks(held, {}, [0, 1], gathered[2], first, wanted)
    near_found = combine(near_found, latter)
    last = []
    for k in range(PARTS):
        if k < PARTS // 2:
            last.append((lax.ppermute(up[k], "z", around(8, 1)), PARTS * 4 + k))
        else:
            last.append((lax.ppermute(down[k], "z", around(8, -1)), PARTS * 4 + k))
    early = gathered[1] + gathered[2]
    (wanted_far,) = after((wanted,), (near_found,))
    far_found, far = score_blocks({(3,): diagonal}, {2: across}, [3, 2], early, first, wanted_far)
    found = jnp.concatenate([near_found, far_found])
    stores, every = held | {(2,): far, (3,): diagonal}, [0, 1, 2, 3]
    (latter,) = score_blocks(stores, {}, every, gathered[3], first, wanted_far)
    (wanted_last,) = after((wanted,), (latter,))
    (message,) = score_blocks(
        stores, {}, every, gathered[0] + last, first, wanted_last, (found, latter), (0,)
    )
    message = message.reshape(32, 1, 128)
    received = lax.all_to_all(
        message, ("yl", "c", "yh", "x"), split_axis=0, concat_axis=0, tiled=True
    ).reshape(32, 128)
    partial, target_logit = received[:, :64], jnp.sum(received[:, 64:], axis=0)
    highest = jnp.max(partial, axis=0)
    summed = jnp.sum(jnp.exp(partial - highest[None]), axis=0)
    slice_tokens = token_count // 8
    confidence = (target_logit - (highest + jnp.log(summed))).reshape(shadow_count, slice_tokens)

    member_tokens = jnp.repeat(membership, SEQ, axis=1)
    outside = (
        1 - lax.dynamic_slice_in_dim(member_tokens, vocab_index * slice_tokens, slice_tokens, 1)
    ).astype(jnp.float32)
    weighted = outside * confidence
    sums = jnp.concatenate([jnp.sum(weighted, axis=0), jnp.sum(weighted * confidence, axis=0)])
    copies = jnp.broadcast_to(sums, (32, 1, 2 * slice_tokens))
    total = jnp.sum(
        lax.all_to_all(copies, ("z", "yl", "c"), split_axis=0, concat_axis=0, tiled=True), axis=(0, 1)
    )
    first_moment, second_moment = total[:slice_tokens], total[slice_tokens:]
    out_count = 64 - outside
    out_mean = (first_moment[None, :] - weighted) / out_count
    out_variance = (
        second_moment[None, :] - weighted * confidence
    ) / out_count - out_mean * out_mean
    return (confidence - out_mean) * lax.rsqrt(jnp.maximum(out_variance, 0.0) + VAR_FLOOR)


def solution(mesh):
    parts = Mesh(mesh.devices.reshape(8, 2, 2, 2, 4), ("z", "yl", "c", "yh", "x"))
    shadow, vocab = ("z", "yl", "c"), ("yh", "x")

    return jax.shard_map(
        per_device,
        mesh=parts,
        in_specs=(P(shadow, None, None), P(), P(shadow, None), P(shadow + vocab, None)),
        out_specs=P(shadow, vocab),
        check_vma=False,
    )
```

```python
import functools

import jax
import jax.numpy as jnp
from jax import lax
from jax.experimental import pallas as pl
from jax.experimental.pallas import tpu as pltpu
from jax.sharding import Mesh, PartitionSpec as P


SEQ = 32


NEG_FILL = -1e30
VAR_FLOOR = 0.5
PARTS = 2


def around(size, step):
    return [(k, (k + step) % size) for k in range(size)]


def across_y():
    place = lambda y, core: (y % 2 * 2 + core) * 2 + y // 2
    return [(place(y, core), place((y + 2 * core - 1) % 4, core)) for y in range(4) for core in (0, 1)]


def scores_kernel(done_near, before_count, fresh_counts, held, blocks, places, *refs):
    refs = list(refs)
    first_ref, wanted_ref = refs.pop(0), refs.pop(0)
    before = [refs.pop(0) for _ in range(before_count)]
    place_of = {}
    for group in held:
        ref = refs.pop(0)
        place_of |= {b: ref.at[n] if len(ref.shape) == 4 else ref for n, b in enumerate(group)}
    fresh_refs = {b: refs.pop(0) for b in fresh_counts}
    head_refs = [refs.pop(0) for _ in places]
    out = refs.pop(0)
    copies = {}
    if fresh_counts:
        kept, sems = refs
        place_of |= {b: kept.at[n] for n, b in enumerate(fresh_counts)}
        for b, ref in fresh_refs.items():
            for half in range(2):
                tokens = pl.ds(64 * half, 64)
                copies[b, half] = pltpu.make_async_copy(
                    ref.at[:, tokens],
                    place_of[b].at[:, tokens],
                    sems.at[len(copies)],
                )
        queue = list(copies.values())
        for copy in queue[:2]:
            copy.start()
        queue = queue[2:]

    def grouped(b):
        groups, size = [[]], 0
        for place, ref in zip(places, head_refs):
            if b < 2 and place in done_near:
                continue
            if size + ref.shape[0] > 256:
                groups.append([])
                size = 0
            groups[-1].append((place, ref))
            size += ref.shape[0]
        return groups

    for b in blocks:
        n = sorted(blocks).index(b)
        for half in range(2):
            if (b, half) in copies:
                copies[b, half].wait()
                if queue:
                    queue.pop(0).start()
            rows = jnp.concatenate(
                [
                    place_of[b][k, 16 * v : 16 * v + 16, :]
                    for v in range(4 * half, 4 * half + 4)
                    for k in range(4)
                ],
                axis=0,
            )
            lanes = slice(256 * half, 256 * half + 256)
            wanted = wanted_ref[0:1, lanes]
            pieces = []
            for group in grouped(b):
                head = jnp.concatenate([ref[...] for _, ref in group], axis=0)
                logits = lax.dot_general(
                    head, rows, (((1,), (1,)), ((), ())), preferred_element_type=jnp.float32
                )
                at = 0
                for place, ref in group:
                    part = logits[at : at + ref.shape[0]]
                    at += ref.shape[0]
                    place_in_piece = lax.broadcasted_iota(jnp.int32, part.shape, 0)
                    pieces.append((part, place_in_piece == wanted - first_ref[place]))
            target_logit = sum(
                jnp.sum(jnp.where(hit, part, 0.0), axis=0, keepdims=True) for part, hit in pieces
            )
            others = [jnp.where(hit, NEG_FILL, part) for part, hit in pieces]
            highest = functools.reduce(
                jnp.maximum, [jnp.max(part, axis=0, keepdims=True) for part in others]
            )
            summed = sum(
                jnp.sum(jnp.exp(part - highest), axis=0, keepdims=True) for part in others
            )
            if not before:
                out[n, 0:1, lanes] = highest
                out[n, 1:2, lanes] = summed
                out[n, 2:3, lanes] = target_logit
                continue
            for ref in before:
                earlier, raised = ref[n, 0:1, lanes], jnp.maximum(highest, ref[n, 0:1, lanes])
                summed = summed * jnp.exp(highest - raised) + ref[n, 1:2, lanes] * jnp.exp(
                    earlier - raised
                )
                highest = raised
                target_logit = target_logit + ref[n, 2:3, lanes]
            total, message = highest + jnp.log(summed), []
            left = lax.broadcasted_iota(jnp.int32, (1, 128), 1) < 64
            for k in range(2):
                part, hit = total[:, 128 * k : 128 * k + 128], target_logit[:, 128 * k : 128 * k + 128]
                message.append(jnp.where(left, part, pltpu.roll(hit, 64, 1)))
                message.append(jnp.where(left, pltpu.roll(part, 64, 1), hit))
            owner = first_ref[first_ref.shape[0] - 1] ^ b
            out[owner, 4 * half : 4 * half + 4, :] = jnp.concatenate(message, axis=0)


def score_blocks(stores, fresh, blocks, pieces, first, wanted, before=(), done_near=()):
    heads = [head for head, _ in pieces]
    vmem = pl.BlockSpec(memory_space=pltpu.VMEM)
    head_rows = sum(head.shape[0] for head in heads)
    shape = (4, 8, 128) if before else (len(blocks), 3, 512)
    outs = [jax.ShapeDtypeStruct(shape, jnp.float32)]
    if fresh:
        outs.append(jax.ShapeDtypeStruct((len(fresh), 4, 128, 2048), jnp.bfloat16))
    results = pl.pallas_call(
        functools.partial(
            scores_kernel, done_near, len(before), list(fresh), list(stores), blocks, [place for _, place in pieces]
        ),
        in_specs=[pl.BlockSpec(memory_space=pltpu.SMEM), vmem]
        + [vmem] * (len(before) + len(stores))
        + [pl.BlockSpec(memory_space=pltpu.HBM)] * len(fresh)
        + [vmem] * len(heads),
        out_specs=[vmem] * len(outs),
        out_shape=outs,
        scratch_shapes=[pltpu.SemaphoreType.DMA((2 * len(fresh),))] if fresh else [],
        compiler_params=pltpu.CompilerParams(vmem_limit_bytes=12 << 20),
        cost_estimate=pl.CostEstimate(
            flops=2 * 512 * len(blocks) * head_rows * 2048,
            bytes_accessed=2 * 2048 * (head_rows + 512 * len(blocks)),
            transcendentals=512 * len(blocks) * head_rows,
        ),
    )(
        first,
        wanted,
        *before,
        *stores.values(),
        *[pltpu.with_memory_space_constraint(rows, pltpu.HBM) for rows in fresh.values()],
        *heads,
    )
    return results


def wanted_kernel(targets_ref, wanted_ref):
    targets = jnp.broadcast_to(targets_ref[...], (8, 128))
    turned = [targets] + [pltpu.roll(targets, 16 * k, 1) for k in range(1, 8)]
    place = lax.broadcasted_iota(jnp.int32, (8, 128), 1) // 16
    for quarter in range(4):
        lanes = targets
        for s in range(8):
            lanes = jnp.where(place == s, turned[(s - 2 * quarter - s // 4) % 8], lanes)
        wanted_ref[0:1, 128 * quarter : 128 * quarter + 128] = lanes[0:1]


def wanted_rows(targets):
    vmem = pl.BlockSpec(memory_space=pltpu.VMEM)
    return pl.pallas_call(
        wanted_kernel,
        in_specs=[vmem],
        out_specs=vmem,
        out_shape=jax.ShapeDtypeStruct((1, 512), jnp.int32),
        compiler_params=pltpu.CompilerParams(vmem_limit_bytes=4 << 20),
    )(targets.reshape(1, 128))


def after(values, others):
    return lax.optimization_barrier((*values, *others))[: len(values)]


def combine(earlier, latter):
    raised = jnp.maximum(earlier[:, 0], latter[:, 0])
    summed = earlier[:, 1] * jnp.exp(earlier[:, 0] - raised) + latter[:, 1] * jnp.exp(
        latter[:, 0] - raised
    )
    return jnp.stack([raised, summed, earlier[:, 2] + latter[:, 2]], axis=1)


def per_device(hidden, targets, membership, unembedding):
    shadow_count, token_count, _ = hidden.shape
    head_rows = unembedding.shape[0]
    z, yl, core = lax.axis_index("z"), lax.axis_index("yl"), lax.axis_index("c")
    vocab_index = lax.axis_index(("yh", "x"))
    part_rows = head_rows // PARTS

    place = jnp.arange(8 * PARTS + 1, dtype=jnp.int32)
    source = (((z - place // PARTS) & 7) * 4 + yl * 2 + core) * 8 + vocab_index
    first = source * head_rows + place % PARTS * part_rows
    first = jnp.where(jnp.arange(8 * PARTS + 1) < 8 * PARTS, first, yl * 2 + core)

    swap = [(0, 1), (1, 0)]
    up, down, gathered = [unembedding], [unembedding], [[(unembedding, 0)]]

    def forward(step):
        for k in range(len(up)):
            up[k] = lax.ppermute(up[k], "z", around(8, 1))
            down[k] = lax.ppermute(down[k], "z", around(8, -1))
        gathered.append(
            [(rows, PARTS * step + k) for k, rows in enumerate(up)]
            + [(rows, PARTS * (8 - step) + k) for k, rows in enumerate(down)]
        )

    forward(1)
    beside = lax.ppermute(hidden, "c", swap)
    across = lax.ppermute(hidden, ("yl", "c", "yh"), across_y())
    wanted = wanted_rows(targets)
    near_found, near = score_blocks({(1,): beside}, {0: hidden}, [1, 0], gathered[0], first, wanted)
    up = [up[0][k * part_rows : (k + 1) * part_rows] for k in range(PARTS)]
    down = [down[0][k * part_rows : (k + 1) * part_rows] for k in range(PARTS)]
    forward(2)
    held = {(0,): near, (1,): beside}
    (latter,) = score_blocks(held, {}, [0, 1], gathered[1], first, wanted)
    near_found = combine(near_found, latter)
    forward(3)
    diagonal = lax.ppermute(across, "c", swap)
    (latter,) = score_blocks(held, {}, [0, 1], gathered[2], first, wanted)
    near_found = combine(near_found, latter)
    last = []
    for k in range(PARTS):
        if k < PARTS // 2:
            last.append((lax.ppermute(up[k], "z", around(8, 1)), PARTS * 4 + k))
        else:
            last.append((lax.ppermute(down[k], "z", around(8, -1)), PARTS * 4 + k))
    early = gathered[1] + gathered[2]
    (wanted_far,) = after((wanted,), (near_found,))
    far_found, far = score_blocks({(3,): diagonal}, {2: across}, [3, 2], early, first, wanted_far)
    found = jnp.concatenate([near_found, far_found])
    stores, every = held | {(2,): far, (3,): diagonal}, [0, 1, 2, 3]
    (latter,) = score_blocks(stores, {}, every, gathered[3], first, wanted_far)
    (wanted_last,) = after((wanted,), (latter,))
    (message,) = score_blocks(
        stores, {}, every, gathered[0] + last, first, wanted_last, (found, latter), (0,)
    )
    message = message.reshape(32, 1, 128)
    received = lax.all_to_all(
        message, ("yl", "c", "yh", "x"), split_axis=0, concat_axis=0, tiled=True
    ).reshape(32, 128)
    partial, target_logit = received[:, :64], jnp.sum(received[:, 64:], axis=0)
    highest = jnp.max(partial, axis=0)
    summed = jnp.sum(jnp.exp(partial - highest[None]), axis=0)
    slice_tokens = token_count // 8
    confidence = (target_logit - (highest + jnp.log(summed))).reshape(shadow_count, slice_tokens)

    membership, position = after((membership, vocab_index), (received,))
    mine = jnp.arange(token_count // SEQ) == position >> (SEQ // slice_tokens - 1)
    outside = (1 - jnp.sum(jnp.where(mine, membership, 0), axis=1, keepdims=True)).astype(jnp.float32)
    weighted = outside * confidence
    sums = jnp.concatenate([jnp.sum(weighted, axis=0), jnp.sum(weighted * confidence, axis=0)])
    sums, out_count, weighted, confidence = lax.optimization_barrier(
        (sums, 64 - outside, weighted, confidence)
    )
    copies = jnp.broadcast_to(sums, (32, 1, 2 * slice_tokens))
    total = jnp.sum(
        lax.all_to_all(copies, ("z", "yl", "c"), split_axis=0, concat_axis=0, tiled=True), axis=(0, 1)
    )
    first_moment, second_moment = total[:slice_tokens], total[slice_tokens:]
    out_mean = (first_moment[None, :] - weighted) / out_count
    out_variance = (
        second_moment[None, :] - weighted * confidence
    ) / out_count - out_mean * out_mean
    return (confidence - out_mean) * lax.rsqrt(jnp.maximum(out_variance, 0.0) + VAR_FLOOR)


def solution(mesh):
    parts = Mesh(mesh.devices.reshape(8, 2, 2, 2, 4), ("z", "yl", "c", "yh", "x"))
    shadow, vocab = ("z", "yl", "c"), ("yh", "x")

    return jax.shard_map(
        per_device,
        mesh=parts,
        in_specs=(P(shadow, None, None), P(), P(shadow, None), P(shadow + vocab, None)),
        out_specs=P(shadow, vocab),
        check_vma=False,
    )
```

```python
import functools

import jax
import jax.numpy as jnp
from jax import lax
from jax.experimental import pallas as pl
from jax.experimental.pallas import tpu as pltpu
from jax.sharding import Mesh, PartitionSpec as P


SEQ = 32


NEG_FILL = -1e30
VAR_FLOOR = 0.5
PARTS = 2


def around(size, step):
    return [(k, (k + step) % size) for k in range(size)]


def across_y():
    place = lambda y, core: (y % 2 * 2 + core) * 2 + y // 2
    return [(place(y, core), place((y + 2 * core - 1) % 4, core)) for y in range(4) for core in (0, 1)]


def scores_kernel(done_near, before_count, fresh_counts, held, blocks, places, *refs):
    refs = list(refs)
    first_ref, wanted_ref = refs.pop(0), refs.pop(0)
    before = [refs.pop(0) for _ in range(before_count)]
    place_of = {}
    for group in held:
        ref = refs.pop(0)
        place_of |= {b: ref.at[n] if len(ref.shape) == 4 else ref for n, b in enumerate(group)}
    fresh_refs = {b: refs.pop(0) for b in fresh_counts}
    head_refs = [refs.pop(0) for _ in places]
    out = refs.pop(0)
    copies = {}
    if fresh_counts:
        kept, sems = refs
        place_of |= {b: kept.at[n] for n, b in enumerate(fresh_counts)}
        for b, ref in fresh_refs.items():
            for half in range(2):
                tokens = pl.ds(64 * half, 64)
                copies[b, half] = pltpu.make_async_copy(
                    ref.at[:, tokens],
                    place_of[b].at[:, tokens],
                    sems.at[len(copies)],
                )
        queue = list(copies.values())
        for copy in queue[:2]:
            copy.start()
        queue = queue[2:]

    def grouped(b):
        groups, size = [[]], 0
        for place, ref in zip(places, head_refs):
            if b < 2 and place in done_near:
                continue
            if size + ref.shape[0] > 256:
                groups.append([])
                size = 0
            groups[-1].append((place, ref))
            size += ref.shape[0]
        return groups

    for b in blocks:
        n = sorted(blocks).index(b)
        for half in range(2):
            if (b, half) in copies:
                copies[b, half].wait()
                if queue:
                    queue.pop(0).start()
            rows = jnp.concatenate(
                [
                    place_of[b][k, 16 * v : 16 * v + 16, :]
                    for v in range(4 * half, 4 * half + 4)
                    for k in range(4)
                ],
                axis=0,
            )
            lanes = slice(256 * half, 256 * half + 256)
            wanted = wanted_ref[0:1, lanes]
            pieces = []
            for group in grouped(b):
                head = jnp.concatenate([ref[...] for _, ref in group], axis=0)
                logits = lax.dot_general(
                    head, rows, (((1,), (1,)), ((), ())), preferred_element_type=jnp.float32
                )
                at = 0
                for place, ref in group:
                    part = logits[at : at + ref.shape[0]]
                    at += ref.shape[0]
                    place_in_piece = lax.broadcasted_iota(jnp.int32, part.shape, 0)
                    pieces.append((part, place_in_piece == wanted - first_ref[place]))
            target_logit = sum(
                jnp.sum(jnp.where(hit, part, 0.0), axis=0, keepdims=True) for part, hit in pieces
            )
            others = [jnp.where(hit, NEG_FILL, part) for part, hit in pieces]
            highest = functools.reduce(
                jnp.maximum, [jnp.max(part, axis=0, keepdims=True) for part in others]
            )
            summed = sum(
                jnp.sum(jnp.exp(part - highest), axis=0, keepdims=True) for part in others
            )
            if not before:
                out[n, 0:1, lanes] = highest
                out[n, 1:2, lanes] = summed
                out[n, 2:3, lanes] = target_logit
                continue
            for ref in before:
                m = n if ref.shape[0] == 4 else n - (2 if ref is before[-2] else 0)
                if not 0 <= m < ref.shape[0]:
                    continue
                earlier, raised = ref[m, 0:1, lanes], jnp.maximum(highest, ref[m, 0:1, lanes])
                summed = summed * jnp.exp(highest - raised) + ref[m, 1:2, lanes] * jnp.exp(
                    earlier - raised
                )
                highest = raised
                target_logit = target_logit + ref[m, 2:3, lanes]
            total, message = highest + jnp.log(summed), []
            left = lax.broadcasted_iota(jnp.int32, (1, 128), 1) < 64
            for k in range(2):
                part, hit = total[:, 128 * k : 128 * k + 128], target_logit[:, 128 * k : 128 * k + 128]
                message.append(jnp.where(left, part, pltpu.roll(hit, 64, 1)))
                message.append(jnp.where(left, pltpu.roll(part, 64, 1), hit))
            owner = first_ref[first_ref.shape[0] - 1] ^ b
            out[owner, 4 * half : 4 * half + 4, :] = jnp.concatenate(message, axis=0)


def score_blocks(stores, fresh, blocks, pieces, first, wanted, before=(), done_near=()):
    heads = [head for head, _ in pieces]
    vmem = pl.BlockSpec(memory_space=pltpu.VMEM)
    head_rows = sum(head.shape[0] for head in heads)
    shape = (4, 8, 128) if before else (len(blocks), 3, 512)
    outs = [jax.ShapeDtypeStruct(shape, jnp.float32)]
    if fresh:
        outs.append(jax.ShapeDtypeStruct((len(fresh), 4, 128, 2048), jnp.bfloat16))
    results = pl.pallas_call(
        functools.partial(
            scores_kernel, done_near, len(before), list(fresh), list(stores), blocks, [place for _, place in pieces]
        ),
        in_specs=[pl.BlockSpec(memory_space=pltpu.SMEM), vmem]
        + [vmem] * (len(before) + len(stores))
        + [pl.BlockSpec(memory_space=pltpu.HBM)] * len(fresh)
        + [vmem] * len(heads),
        out_specs=[vmem] * len(outs),
        out_shape=outs,
        scratch_shapes=[pltpu.SemaphoreType.DMA((2 * len(fresh),))] if fresh else [],
        compiler_params=pltpu.CompilerParams(vmem_limit_bytes=12 << 20),
        cost_estimate=pl.CostEstimate(
            flops=2 * 512 * len(blocks) * head_rows * 2048,
            bytes_accessed=2 * 2048 * (head_rows + 512 * len(blocks)),
            transcendentals=512 * len(blocks) * head_rows,
        ),
    )(
        first,
        wanted,
        *before,
        *stores.values(),
        *[pltpu.with_memory_space_constraint(rows, pltpu.HBM) for rows in fresh.values()],
        *heads,
    )
    return results


def wanted_kernel(targets_ref, wanted_ref):
    targets = jnp.broadcast_to(targets_ref[...], (8, 128))
    turned = [targets] + [pltpu.roll(targets, 16 * k, 1) for k in range(1, 8)]
    place = lax.broadcasted_iota(jnp.int32, (8, 128), 1) // 16
    for quarter in range(4):
        lanes = targets
        for s in range(8):
            lanes = jnp.where(place == s, turned[(s - 2 * quarter - s // 4) % 8], lanes)
        wanted_ref[0:1, 128 * quarter : 128 * quarter + 128] = lanes[0:1]


def wanted_rows(targets):
    vmem = pl.BlockSpec(memory_space=pltpu.VMEM)
    return pl.pallas_call(
        wanted_kernel,
        in_specs=[vmem],
        out_specs=vmem,
        out_shape=jax.ShapeDtypeStruct((1, 512), jnp.int32),
        compiler_params=pltpu.CompilerParams(vmem_limit_bytes=4 << 20),
    )(targets.reshape(1, 128))


def after(values, others):
    return lax.optimization_barrier((*values, *others))[: len(values)]


def combine(earlier, latter):
    raised = jnp.maximum(earlier[:, 0], latter[:, 0])
    summed = earlier[:, 1] * jnp.exp(earlier[:, 0] - raised) + latter[:, 1] * jnp.exp(
        latter[:, 0] - raised
    )
    return jnp.stack([raised, summed, earlier[:, 2] + latter[:, 2]], axis=1)


def per_device(hidden, targets, membership, unembedding):
    shadow_count, token_count, _ = hidden.shape
    head_rows = unembedding.shape[0]
    z, yl, core = lax.axis_index("z"), lax.axis_index("yl"), lax.axis_index("c")
    vocab_index = lax.axis_index(("yh", "x"))
    part_rows = head_rows // PARTS

    place = jnp.arange(8 * PARTS + 1, dtype=jnp.int32)
    source = (((z - place // PARTS) & 7) * 4 + yl * 2 + core) * 8 + vocab_index
    first = source * head_rows + place % PARTS * part_rows
    first = jnp.where(jnp.arange(8 * PARTS + 1) < 8 * PARTS, first, yl * 2 + core)

    swap = [(0, 1), (1, 0)]
    up, down, gathered = [unembedding], [unembedding], [[(unembedding, 0)]]

    def forward(step):
        for k in range(len(up)):
            up[k] = lax.ppermute(up[k], "z", around(8, 1))
            down[k] = lax.ppermute(down[k], "z", around(8, -1))
        gathered.append(
            [(rows, PARTS * step + k) for k, rows in enumerate(up)]
            + [(rows, PARTS * (8 - step) + k) for k, rows in enumerate(down)]
        )

    forward(1)
    beside = lax.ppermute(hidden, "c", swap)
    across = lax.ppermute(hidden, ("yl", "c", "yh"), across_y())
    wanted = wanted_rows(targets)
    near_found, near = score_blocks({(1,): beside}, {0: hidden}, [1, 0], gathered[0], first, wanted)
    up = [up[0][k * part_rows : (k + 1) * part_rows] for k in range(PARTS)]
    down = [down[0][k * part_rows : (k + 1) * part_rows] for k in range(PARTS)]
    forward(2)
    held = {(0,): near, (1,): beside}
    (latter,) = score_blocks(held, {}, [0, 1], gathered[1], first, wanted)
    near_found = combine(near_found, latter)
    forward(3)
    diagonal = lax.ppermute(across, "c", swap)
    (latter,) = score_blocks(held, {}, [0, 1], gathered[2], first, wanted)
    near_found = combine(near_found, latter)
    last = []
    for k in range(PARTS):
        if k < PARTS // 2:
            last.append((lax.ppermute(up[k], "z", around(8, 1)), PARTS * 4 + k))
        else:
            last.append((lax.ppermute(down[k], "z", around(8, -1)), PARTS * 4 + k))
    early = gathered[1] + gathered[2]
    (wanted_far,) = after((wanted,), (near_found,))
    far_found, far = score_blocks({(3,): diagonal}, {2: across}, [3, 2], early, first, wanted_far)
    stores, every = held | {(2,): far, (3,): diagonal}, [0, 1, 2, 3]
    (latter,) = score_blocks(stores, {}, every, gathered[3], first, wanted_far)
    (wanted_last,) = after((wanted,), (latter,))
    (message,) = score_blocks(
        stores, {}, every, gathered[0] + last, first, wanted_last, (near_found, far_found, latter), (0,)
    )
    message = message.reshape(32, 1, 128)
    received = lax.all_to_all(
        message, ("yl", "c", "yh", "x"), split_axis=0, concat_axis=0, tiled=True
    ).reshape(32, 128)
    partial, target_logit = received[:, :64], jnp.sum(received[:, 64:], axis=0)
    highest = jnp.max(partial, axis=0)
    summed = jnp.sum(jnp.exp(partial - highest[None]), axis=0)
    slice_tokens = token_count // 8
    confidence = (target_logit - (highest + jnp.log(summed))).reshape(shadow_count, slice_tokens)

    membership, position = after((membership, vocab_index), (received,))
    mine = jnp.arange(token_count // SEQ) == position >> (SEQ // slice_tokens - 1)
    outside = (1 - jnp.sum(jnp.where(mine, membership, 0), axis=1, keepdims=True)).astype(jnp.float32)
    weighted = outside * confidence
    sums = jnp.concatenate([jnp.sum(weighted, axis=0), jnp.sum(weighted * confidence, axis=0)])
    sums, out_count, weighted, confidence = lax.optimization_barrier(
        (sums, 64 - outside, weighted, confidence)
    )
    copies = jnp.broadcast_to(sums, (32, 1, 2 * slice_tokens))
    total = jnp.sum(
        lax.all_to_all(copies, ("z", "yl", "c"), split_axis=0, concat_axis=0, tiled=True), axis=(0, 1)
    )
    first_moment, second_moment = total[:slice_tokens], total[slice_tokens:]
    out_mean = (first_moment[None, :] - weighted) / out_count
    out_variance = (
        second_moment[None, :] - weighted * confidence
    ) / out_count - out_mean * out_mean
    return (confidence - out_mean) * lax.rsqrt(jnp.maximum(out_variance, 0.0) + VAR_FLOOR)


def solution(mesh):
    parts = Mesh(mesh.devices.reshape(8, 2, 2, 2, 4), ("z", "yl", "c", "yh", "x"))
    shadow, vocab = ("z", "yl", "c"), ("yh", "x")

    return jax.shard_map(
        per_device,
        mesh=parts,
        in_specs=(P(shadow, None, None), P(), P(shadow, None), P(shadow + vocab, None)),
        out_specs=P(shadow, vocab),
        check_vma=False,
    )
```
